32 devices in a mesh: ctx: 2 (over x), tp: 4 (over z), dp: 4 (over y, core).
Axes of the slice: x: 2, y: 2, z: 4, core: 2. Of those that a mesh axis runs over, the one named last changes fastest.
Arguments:
- queries: bfloat16 [4, 256, 4096], P('dp', 'ctx', 'tp'), may hold values from -6 to 6
- keys: bfloat16 [4, 2, 4, 32, 128, 128], P('dp', None, 'tp', 'ctx'), may hold values from -6 to 6
- values: bfloat16 [4, 2, 4, 32, 128, 128], P('dp', None, 'tp', 'ctx'), may hold values from -6 to 6
- cotangent: bfloat16 [4, 256, 4096], P('dp', 'ctx', 'tp'), may hold values from -6 to 6
- lengths: int32 [4, 4, 2], P('dp'), may hold values from 16 to 128
Outputs:
- attended: bfloat16 [4, 256, 4096], P('dp', 'ctx', 'tp')
- grad_queries: bfloat16 [4, 256, 4096], P('dp', 'ctx', 'tp')
- grad_keys: bfloat16 [4, 2, 4, 32, 128, 128], P('dp', None, 'tp', 'ctx')
- grad_values: bfloat16 [4, 2, 4, 32, 128, 128], P('dp', None, 'tp', 'ctx')
The draws below stay inside these ranges and needn't reach their ends.
Inputs may be any that keep to these rules, and one draw needn't show every extreme that they name: Neighbour n of span u has its first lengths[u, n] tokens live; the others are padding.
All inputs are finite; a program needn't handle non-finite values.
Results may differ from the reference program's by a relative error of at most 0.012.
The reference program's roundings to bfloat16 on the way count: a program that leaves them out, or rounds other values in their place, can miss the bound.
Values may be sent and summed in bfloat16 or wider, within the bound.
A program may use at most 64 MiB of HBM per device.

```python
import math
import jax
import jax.numpy as jnp
from jax import lax

HEADS = 32
DH = 128
SPAN = 64
NBR = 2
NEIGH = 128
TOK_DEV = 128
SEQ = 256
SPANS = 4
PASS = 4
BATCH = 4
N_CTX = 2


def draw_queries(key, part):
    shape_all = (BATCH, SEQ, HEADS * DH)
    sampled = jnp.clip(jax.random.normal(key, shape_all, jnp.float32), -6.0, 6.0)
    return sampled.astype(jnp.bfloat16)


def draw_keys(key, part):
    block_count = SEQ // TOK_DEV
    shape_all = (BATCH, block_count, PASS, HEADS, NEIGH, DH)
    sampled = jnp.clip(jax.random.normal(jax.random.fold_in(key, 23), shape_all, jnp.float32), -6.0, 6.0)
    return sampled.astype(jnp.bfloat16)


def plant(drawn, rng, least, top_value):
    longest = drawn.shape.index(max(drawn.shape))
    spots = []
    for shift in (0, 1):
        where = [jax.random.randint(jax.random.fold_in(rng, axis), (), 0, length) for axis, length in enumerate(drawn.shape)]
        where[longest] = (where[longest] + shift) % drawn.shape[longest]
        spots.append(tuple(where))
    return drawn.at[spots[0]].set(least).at[spots[1]].set(top_value)


def steps_of(rng, dims, cuts, smallest, high):
    def one(position, parts):
        draws = jax.random.uniform(jax.random.fold_in(jax.random.fold_in(rng, 6), position), (parts,), jnp.float32, smallest / len(cuts), high / len(cuts))
        return jnp.repeat(jnp.exp(draws), dims[position] // parts).reshape((-1,) + (1,) * (len(dims) - position - 1))

    loudness = one(*cuts[0])
    for cut in cuts[1:]:
        loudness = loudness * one(*cut)
    return loudness


def scatter_about(stream_key, shape, scale, most, cuts=(), held_as=jnp.bfloat16):
    gain = steps_of(stream_key, shape, cuts, -0.22, 0.18) if cuts else 1.0
    drawn = jax.random.normal(stream_key, shape, jnp.float32) * scale * gain
    return jnp.minimum(jnp.maximum(drawn, -most), most).astype(held_as)


def setup_inputs(seed: int = 0) -> dict:
    seeds = jax.random.split(jax.random.key(seed), 6)
    queries = draw_queries(jax.random.fold_in(seeds[5], 71), 0)
    keys = draw_keys(jax.random.fold_in(seeds[5], 71), 0)
    values = scatter_about(seeds[2], (BATCH, N_CTX, PASS, HEADS, NEIGH, DH), 1.0, 6.0, ((0, 4), (2, 4), (3, 2)))
    cotangent = scatter_about(seeds[3], (BATCH, SEQ, HEADS * DH), 1.0, 6.0, ((0, 4), (1, 2), (2, 4)))
    lengths = plant(jax.random.randint(seeds[4], (BATCH, SPANS, NBR), NEIGH // 8, NEIGH + 1), jax.random.fold_in(seeds[4], 1), NEIGH // 8, NEIGH).astype(jnp.int32)
    return dict(queries=queries, keys=keys, values=values, cotangent=cotangent, lengths=lengths)


def rotate(tensor, direction):
    middle = tensor.shape[-1] // 2
    frequency = 10000.0 ** (-2.0 * jnp.arange(middle, dtype=jnp.float32) / tensor.shape[-1])
    angles = jnp.arange(tensor.shape[-2], dtype=jnp.float32)[:, None] * frequency[None, :]
    cosine = jnp.cos(angles)
    sine_part = direction * jnp.sin(angles)
    lower_part = tensor[..., :middle].astype(jnp.float32)
    upper_part = tensor[..., middle:].astype(jnp.float32)
    return jnp.concatenate([lower_part * cosine - upper_part * sine_part, lower_part * sine_part + upper_part * cosine], axis=-1)

def to_bfloat(tensor):
    return lax.optimization_barrier(tensor.astype(jnp.bfloat16)).astype(jnp.float32)

def live_scores(query_rows, key_rows, key_counts):
    scaling = 1.0 / math.sqrt(query_rows.shape[-1])
    scores = jnp.einsum('zhid,zhjd->zhij', query_rows.astype(jnp.float32), key_rows.astype(jnp.float32)) * scaling
    usable = jnp.arange(key_rows.shape[-2])[None, None, None, :] < key_counts[:, None, None, None]
    return jnp.where(usable, scores, -jnp.inf)

def neighbour_forward(query_rows, key_rows, value_rows, key_counts):
    scores = live_scores(query_rows, key_rows, key_counts)
    maxima = lax.optimization_barrier(jnp.max(scores, axis=-1, keepdims=True))
    weights = jnp.exp(scores - maxima)
    totals = lax.optimization_barrier(jnp.sum(weights, axis=-1))
    summed = jnp.einsum('zhij,zhjd->zhid', to_bfloat(weights), value_rows.astype(jnp.float32))
    return (summed / totals[..., None], maxima[..., 0] + jnp.log(totals))

def neighbour_backward(query_rows, key_rows, value_rows, key_counts, grad_rows, log_totals, output_dots):
    scaling = 1.0 / math.sqrt(query_rows.shape[-1])
    scores = live_scores(query_rows, key_rows, key_counts)
    chances = jnp.exp(scores - log_totals[..., None])
    grad_values = jnp.einsum('zhij,zhid->zhjd', to_bfloat(chances), grad_rows.astype(jnp.float32))
    grad_weights = jnp.einsum('zhid,zhjd->zhij', grad_rows.astype(jnp.float32), value_rows.astype(jnp.float32))
    grad_scores = to_bfloat(chances * (grad_weights - output_dots[..., None]) * scaling)
    grad_query = to_bfloat(jnp.einsum('zhij,zhjd->zhid', grad_scores, key_rows.astype(jnp.float32)))
    grad_key = jnp.einsum('zhij,zhid->zhjd', grad_scores, query_rows.astype(jnp.float32))
    return (grad_query, grad_key, grad_values)

def reference(queries, keys, values, cotangent, lengths):
    rim_rows = SPAN - 1
    row_width = HEADS * DH

    def windows(tokens):
        padded = jnp.concatenate([tokens[:, rim_rows:], jnp.zeros((BATCH, rim_rows, row_width), tokens.dtype)], axis=1)
        return padded.reshape(BATCH * SPANS, SPAN, HEADS, DH).transpose(0, 2, 1, 3)
    query_windows = rotate(windows(queries), 1.0).astype(jnp.bfloat16)
    grad_windows = windows(cotangent)
    key_turned = rotate(keys.reshape(BATCH * SPANS, NBR, HEADS, NEIGH, DH), 1.0).astype(jnp.bfloat16)
    value_rows = values.reshape(BATCH * SPANS, NBR, HEADS, NEIGH, DH)
    key_counts = lengths.reshape(BATCH * SPANS, NBR).astype(jnp.int32)

    def span_work(pieces):
        query_one, grad_one, key_one, value_one, counts_one = pieces
        query_pair = jnp.broadcast_to(query_one[None], (NBR,) + query_one.shape)
        grad_pair = jnp.broadcast_to(grad_one[None], (NBR,) + grad_one.shape)
        partial_value, log_parts = neighbour_forward(query_pair, key_one, value_one, counts_one)
        log_whole = jax.nn.logsumexp(log_parts, axis=0)
        attended = lax.optimization_barrier(jnp.sum(jnp.exp(log_parts - log_whole[None])[..., None] * partial_value, axis=0)).astype(jnp.bfloat16)
        output_dots = lax.optimization_barrier(jnp.sum(grad_one.astype(jnp.float32) * attended.astype(jnp.float32), axis=-1))
        grad_query, grad_key, grad_values = neighbour_backward(query_pair, key_one, value_one, counts_one, grad_pair, jnp.broadcast_to(log_whole[None], log_parts.shape), jnp.broadcast_to(output_dots[None], log_parts.shape))
        return (attended, lax.optimization_barrier(jnp.sum(grad_query, axis=0)), grad_key, grad_values.astype(jnp.bfloat16))
    attended, grad_sum, grad_key, grad_values = lax.map(span_work, (query_windows, grad_windows, key_turned, value_rows, key_counts))

    def tokens_of(window_rows):
        flat_rows = window_rows.transpose(0, 2, 1, 3).reshape(BATCH, SEQ, row_width)
        return jnp.concatenate([jnp.zeros((BATCH, rim_rows, row_width), flat_rows.dtype), flat_rows[:, :SEQ - rim_rows]], axis=1)
    grad_windows_out = rotate(grad_sum, -1.0).astype(jnp.bfloat16)
    grad_keys = rotate(grad_key, -1.0).astype(jnp.bfloat16).reshape(keys.shape)
    return (tokens_of(attended), tokens_of(grad_windows_out), grad_keys, grad_values.reshape(values.shape))
```

```python
import functools
import math

import jax
import jax.numpy as jnp
import numpy as np
from jax import lax
from jax.experimental import pallas as pl
from jax.experimental.pallas import tpu as pltpu
from jax.sharding import PartitionSpec as P

DH = 128
SPAN = 64
NBR = 2
TAIL = 16
PAD = TAIL + SPAN
MESH = pl.DeviceIdType.MESH
BF16 = jnp.bfloat16
F32 = jnp.float32


def rotation_tables(rows):
    frequency = 10000.0 ** (-2.0 * np.arange(DH // 2) / DH)
    frequency = frequency.astype(np.float32)
    angles = np.arange(rows, dtype=np.float32)[:, None] * frequency[None, :]
    cosine, sine = np.cos(angles), np.sin(angles)
    return (
        np.concatenate([cosine, cosine], axis=1).astype(np.float32),
        np.concatenate([-sine, sine], axis=1).astype(np.float32),
    )


def dot(a, b, ca, cb):
    return lax.dot_general(a, b, (((ca,), (cb,)), ((), ())), preferred_element_type=F32)


def kernel(
    n_ctx, n_tp, blocks, hc, ht,
    lengths, queries, cotangent, keys, values, cos_ref, sin_ref,
    att_out, gq_out, gk_out, gv_out,
    rin, kbuf, vbuf, gkbuf, gvbuf, qw, gw, ebuf, pbuf, dpbuf, mtile, stat, pstat, sback, bmain, btail,
    in_send, in_recv, st_send, st_recv, bk_send, bk_recv, kv_sem, out_sem,
):
    g = min(hc, ht)
    nbc, nbt = hc // g, ht // g
    units = n_ctx * nbc
    wide = g * DH
    scale = 1.0 / math.sqrt(DH)
    me_c, me_t = lax.axis_index("ctx"), lax.axis_index("tp")
    w, n = me_t // NBR, me_t % NBR
    tokens = (queries, cotangent)
    unroll = 4 if g % 4 == 0 else 1

    def remote(src, dst, send, recv, c, t):
        return pltpu.make_async_remote_copy(
            src_ref=src, dst_ref=dst, send_sem=send, recv_sem=recv,
            device_id={"ctx": c, "tp": t}, device_id_type=MESH,
        )

    def arrive(dst, recv):
        pltpu.make_async_copy(dst, dst, recv).wait()

    def is_me(c, t):
        return jnp.logical_and(c == me_c, t == me_t)

    def kv_copies(c):
        return (
            pltpu.make_async_copy(keys.at[c], kbuf.at[c], kv_sem.at[0, c]),
            pltpu.make_async_copy(values.at[c], vbuf.at[c], kv_sem.at[1, c]),
        )

    @pl.loop(0, n_ctx)
    def _(c):
        for copy in kv_copies(c):
            copy.start()

    barrier = pltpu.get_barrier_semaphore()

    @pl.loop(0, n_ctx * n_tp)
    def _(i):
        c, t = i // n_tp, i % n_tp

        @pl.when(jnp.logical_not(is_me(c, t)))
        def _():
            pl.semaphore_signal(barrier, inc=1, device_id={"ctx": c, "tp": t}, device_id_type=MESH)

    pl.semaphore_wait(barrier, n_ctx * n_tp - 1)

    def in_sends(act):
        for t in reversed(range(n_tp)):
            tw = t // NBR
            for kb in range(nbt):
                first = me_t * ht + kb * g
                c = first // hc
                sb = (first % hc) // g
                for a in range(2):
                    for piece in range(2):
                        ok = True
                        if piece == 0:
                            rows, slot, spot = pl.ds((tw + 1) * SPAN - TAIL, TAIL), me_c, pl.ds(0, TAIL)
                        elif tw < blocks - 1:
                            rows, slot, spot = pl.ds((tw + 1) * SPAN, SPAN), me_c, pl.ds(TAIL, SPAN)
                        else:
                            rows, slot, spot = pl.ds(0, SPAN), me_c - 1, pl.ds(TAIL, SPAN)
                            ok = me_c > 0
                        slot = jnp.maximum(slot, 0)
                        src = tokens[a].at[rows, pl.ds(kb * wide, wide)]
                        unit = slot * nbc + sb
                        dst = rin.at[a, unit, spot]
                        send, recv = in_send.at[a, t, kb, piece], in_recv.at[a, unit, piece]
                        act(src, dst, send, recv, c, t, ok)

    def start(src, dst, send, recv, c, t, ok):
        mine = is_me(c, t)

        @pl.when(jnp.logical_and(ok, mine))
        def _():
            pltpu.make_async_copy(src, dst, recv).start()

        @pl.when(jnp.logical_and(ok, jnp.logical_not(mine)))
        def _():
            remote(src, dst, send, recv, c, t).start()

    def sent(src, dst, send, recv, c, t, ok):
        @pl.when(jnp.logical_and(ok, jnp.logical_not(is_me(c, t))))
        def _():
            remote(src, dst, send, recv, c, t).wait_send()

    in_sends(start)

    def rotated(x, rows, sign):
        turned = pltpu.roll(x, DH // 2, 1) * sin_ref[:rows]
        return x * cos_ref[:rows] + (turned if sign > 0 else -turned)

    def order(k):
        return (me_c + k) % n_ctx

    @pl.loop(0, n_ctx)
    def _(k):
        c = order(k)
        for copy in kv_copies(c):
            copy.wait()

        @pl.loop(0, hc // unroll)
        def _(hg):
            for i in range(unroll):
                h = hg * unroll + i
                x = kbuf[c, h].astype(F32)
                kbuf[c, h] = rotated(x, x.shape[0], 1).astype(BF16)

    lane = lax.broadcasted_iota(jnp.int32, (SPAN, DH), 1)
    half = DH // 2

    def partner_sends(unit, act):
        for i in range(1, NBR):
            t = w * NBR + (n + i) % NBR
            copy = remote(
                stat.at[unit], pstat.at[unit, i - 1], st_send.at[unit, i - 1], st_recv.at[unit, i - 1], me_c, t
            )
            act(copy)

    @pl.loop(0, units)
    def _(k):
        c = order(k // nbc)
        sb = k % nbc
        unit = c * nbc + sb
        missing = jnp.logical_and(w == blocks - 1, c == n_ctx - 1)
        for a in range(2):
            arrive(rin.at[a, unit, pl.ds(0, TAIL)], in_recv.at[a, unit, 0])

            @pl.when(jnp.logical_not(missing))
            def _():
                arrive(rin.at[a, unit, pl.ds(TAIL, SPAN)], in_recv.at[a, unit, 1])

            @pl.when(missing)
            def _():
                rin[a, unit, TAIL:PAD] = jnp.zeros((SPAN, wide), BF16)

        count = lengths[c * blocks + w, n]
        live = lane[:, :] < count
        stat[unit] = jnp.zeros((SPAN, DH), F32)
        mtile[unit] = jnp.zeros((SPAN, DH), F32)

        @pl.loop(0, g // unroll)
        def _(hg):
            lps, ds, ms = [], [], []
            for i in range(unroll):
                hh = hg * unroll + i
                h = sb * g + hh
                at = c * hc + h
                columns = pl.ds(pl.multiple_of(hh * DH, DH), DH)

                def window(a):
                    raw = rin[a, unit, :, columns].astype(F32)
                    return pltpu.roll(raw, PAD - (TAIL - 1), 0)[:SPAN]

                q = rotated(window(0), SPAN, 1).astype(BF16)
                grad32 = window(1)
                grad = grad32.astype(BF16)
                qw[at] = q
                gw[at] = grad
                s = dot(q, kbuf[c, h], 1, 1) * scale
                s = jnp.where(live, s, -jnp.inf)
                m = jnp.max(s, axis=1, keepdims=True)
                e = jnp.exp(s - m)
                total = jnp.sum(e, axis=1, keepdims=True)
                value = vbuf[c, h]
                part = dot(e.astype(BF16), value, 1, 0)
                ebuf[at] = e
                pbuf[at] = part
                dpbuf[at] = dot(grad, value, 1, 1)
                lps.append(m + jnp.log(total))
                ds.append(jnp.sum(grad32 * part, axis=1, keepdims=True) / total)
                ms.append(m)
            st, mt = stat[unit], mtile[unit]
            for i in range(unroll):
                hh = hg * unroll + i
                st = jnp.where(lane == hh, lps[i], st)
                st = jnp.where(lane == hh + half, ds[i], st)
                mt = jnp.where(lane == hh, ms[i], mt)
            stat[unit] = st
            mtile[unit] = mt

        partner_sends(unit, lambda copy: copy.start())

    def back_sends(c, sb, act):
        unit = c * nbc + sb
        first = me_c * hc + sb * g
        t = first // ht
        kb = (first % ht) // g
        columns = pl.ds(pl.multiple_of(kb * wide, DH), wide)
        for a in range(2):
            for piece in range(2):
                if piece == 0:
                    src, dst = sback.at[a, unit, pl.ds(0, TAIL)], btail.at[a, n, w, :, columns]
                    to, ok, recv = c, True, bk_recv.at[a, n, w, kb, 0]
                else:
                    j = jnp.where(w == blocks - 1, 0, w + 1)
                    src, dst = sback.at[a, unit, pl.ds(TAIL, SPAN)], bmain.at[a, n, j, :, columns]
                    to = jnp.where(w == blocks - 1, c + 1, c)
                    ok = to < n_ctx
                    to = jnp.minimum(to, n_ctx - 1)
                    recv = bk_recv.at[a, n, j, kb, 1]
                act(src, dst, bk_send.at[a, unit, piece], recv, to, t, ok)

    def out_copies(c, sb):
        heads = pl.ds(sb * g, g)
        return (
            pltpu.make_async_copy(gkbuf.at[c, heads], gk_out.at[c, heads], out_sem.at[0, c, sb]),
            pltpu.make_async_copy(gvbuf.at[c, heads], gv_out.at[c, heads], out_sem.at[1, c, sb]),
        )

    @pl.loop(0, units)
    def _(k):
        c = order(k // nbc)
        sb = k % nbc
        unit = c * nbc + sb
        partner_sends(unit, lambda copy: copy.wait_recv())
        own = stat[unit]
        others = [pstat[unit, i] for i in range(NBR - 1)]
        top = functools.reduce(jnp.maximum, others, own)
        lse = top + jnp.log(sum(jnp.exp(x - top) for x in [own] + others))
        dots = sum(jnp.exp(x - lse) * pltpu.roll(x, half, 1) for x in [own] + others)
        factor = jnp.exp(mtile[unit] - lse)
        both = jnp.where(lane < half, factor, pltpu.roll(dots, half, 1))

        @pl.loop(0, g // unroll)
        def _(hg):
            for i in range(unroll):
                hh = hg * unroll + i
                h = sb * g + hh
                at = c * hc + h
                columns = pl.ds(pl.multiple_of(hh * DH, DH), DH)
                fac = jnp.sum(jnp.where(lane == hh, both, 0.0), axis=1, keepdims=True)
                dcol = jnp.sum(jnp.where(lane == hh + half, both, 0.0), axis=1, keepdims=True)
                pr = ebuf[at] * fac
                gvbuf[c, h] = dot(pr.astype(BF16), gw[at], 0, 0).astype(BF16)
                gs = (pr * (dpbuf[at] - dcol) * scale).astype(BF16)
                gq = dot(gs, kbuf[c, h], 1, 0)
                gk = dot(gs, qw[at], 0, 0)
                gkbuf[c, h] = rotated(gk, gk.shape[0], -1).astype(BF16)
                att = pbuf[at] * fac
                for a, x in ((0, att), (1, gq)):
                    padded = jnp.concatenate([x, jnp.zeros((TAIL, DH), F32)], axis=0)
                    sback[a, unit, :, columns] = pltpu.roll(padded, TAIL - 1, 0).astype(BF16)

        back_sends(c, sb, start)
        for copy in out_copies(c, sb):
            copy.start()

    shifted_cos = pltpu.roll(cos_ref[:SPAN], SPAN - 1, 0)
    shifted_sin = pltpu.roll(sin_ref[:SPAN], SPAN - 1, 0)
    for j in range(blocks):
        for a in range(2):
            for nn in range(NBR):
                for kb in range(nbt):
                    columns = pl.ds(kb * wide, wide)
                    arrive(btail.at[a, nn, j, :, columns], bk_recv.at[a, nn, j, kb, 0])
                    main = bmain.at[a, nn, j, :, columns]
                    recv = bk_recv.at[a, nn, j, kb, 1]
                    if j > 0:
                        arrive(main, recv)
                    else:
                        @pl.when(me_c > 0)
                        def _():
                            arrive(main, recv)

                        @pl.when(me_c == 0)
                        def _():
                            bmain[a, nn, j, :, kb * wide : (kb + 1) * wide] = jnp.zeros((SPAN, wide), BF16)

        @pl.loop(0, ht)
        def _(h):
            columns = pl.ds(pl.multiple_of(h * DH, DH), DH)

            def gathered(a):
                main = sum(bmain[a, nn, j, :, columns].astype(F32) for nn in range(NBR))
                tail = sum(btail[a, nn, j, :, columns].astype(F32) for nn in range(NBR))
                return jnp.concatenate([main[: SPAN - TAIL], main[SPAN - TAIL :] + tail], axis=0)

            rows = pl.ds(j * SPAN, SPAN)
            att_out[rows, columns] = gathered(0).astype(BF16)
            x = gathered(1)
            x = x * shifted_cos - pltpu.roll(x, DH // 2, 1) * shifted_sin
            gq_out[rows, columns] = x.astype(BF16)

    in_sends(sent)

    @pl.loop(0, units)
    def _(k):
        c, sb = k // nbc, k % nbc
        partner_sends(c * nbc + sb, lambda copy: copy.wait_send())
        back_sends(c, sb, sent)
        for copy in out_copies(c, sb):
            copy.wait()


def shards(n_ctx, n_tp, queries, keys, values, cotangent, lengths):
    rows, width = queries.shape[1:]
    blocks = rows // SPAN
    ht = width // DH
    hc, neigh = keys.shape[3], keys.shape[4]
    assert keys.shape[2] == 1 and blocks * NBR == n_tp
    g = min(hc, ht)
    nbc, nbt = hc // g, ht // g
    units, wide = n_ctx * nbc, g * DH
    cosine, sine = rotation_tables(max(neigh, SPAN))
    kv_shape = (n_ctx, hc, neigh, DH)
    heads = n_ctx * hc
    any_space = pl.BlockSpec(memory_space=pl.ANY)
    vmem = pl.BlockSpec(memory_space=pltpu.VMEM)
    dma = pltpu.SemaphoreType.DMA
    att, gq, gk, gv = pl.pallas_call(
        functools.partial(kernel, n_ctx, n_tp, blocks, hc, ht),
        out_shape=(
            jax.ShapeDtypeStruct((rows, width), BF16),
            jax.ShapeDtypeStruct((rows, width), BF16),
            jax.ShapeDtypeStruct(kv_shape, BF16),
            jax.ShapeDtypeStruct(kv_shape, BF16),
        ),
        in_specs=[pl.BlockSpec(memory_space=pltpu.SMEM), vmem, vmem, any_space, any_space, vmem, vmem],
        out_specs=(vmem, vmem, any_space, any_space),
        scratch_shapes=[
            pltpu.VMEM((2, units, PAD, wide), BF16),
            pltpu.VMEM(kv_shape, BF16),
            pltpu.VMEM(kv_shape, BF16),
            pltpu.VMEM(kv_shape, BF16),
            pltpu.VMEM(kv_shape, BF16),
            pltpu.VMEM((heads, SPAN, DH), BF16),
            pltpu.VMEM((heads, SPAN, DH), BF16),
            pltpu.VMEM((heads, SPAN, neigh), F32),
            pltpu.VMEM((heads, SPAN, DH), F32),
            pltpu.VMEM((heads, SPAN, neigh), F32),
            pltpu.VMEM((units, SPAN, DH), F32),
            pltpu.VMEM((units, SPAN, DH), F32),
            pltpu.VMEM((units, NBR - 1, SPAN, DH), F32),
            pltpu.VMEM((2, units, PAD, wide), BF16),
            pltpu.VMEM((2, NBR, blocks, SPAN, width), BF16),
            pltpu.VMEM((2, NBR, blocks, TAIL, width), BF16),
            dma((2, n_tp, nbt, 2)),
            dma((2, units, 2)),
            dma((units, NBR - 1)),
            dma((units, NBR - 1)),
            dma((2, units, 2)),
            dma((2, NBR, blocks, nbt, 2)),
            dma((2, n_ctx)),
            dma((2, n_ctx, nbc)),
        ],
        compiler_params=pltpu.CompilerParams(
            collective_id=0, has_side_effects=True, vmem_limit_bytes=48 * 1024 * 1024
        ),
    )(
        lengths[0].reshape(-1, NBR),
        queries[0],
        cotangent[0],
        keys.reshape(kv_shape),
        values.reshape(kv_shape),
        jnp.asarray(cosine),
        jnp.asarray(sine),
    )
    return (att[None], gq[None], gk.reshape(keys.shape), gv.reshape(values.shape))


def solution(mesh):
    tok = P("dp", "ctx", "tp")
    kv = P("dp", None, "tp", "ctx", None, None)
    return jax.shard_map(
        functools.partial(shards, mesh.shape["ctx"], mesh.shape["tp"]),
        mesh=mesh,
        in_specs=(tok, kv, kv, tok, P("dp", None, None)),
        out_specs=(tok, tok, kv, kv),
        check_vma=False,
    )
```

```python
import functools
import math

import jax
import jax.numpy as jnp
import numpy as np
from jax import lax
from jax.experimental import pallas as pl
from jax.experimental.pallas import tpu as pltpu
from jax.sharding import PartitionSpec as P

DH = 128
SPAN = 64
NBR = 2
MESH = pl.DeviceIdType.MESH
BF16 = jnp.bfloat16
F32 = jnp.float32


def rotation_tables(rows):
    frequency = 10000.0 ** (-2.0 * np.arange(DH // 2) / DH)
    frequency = frequency.astype(np.float32)
    angles = np.arange(rows, dtype=np.float32)[:, None] * frequency[None, :]
    cosine, sine = np.cos(angles), np.sin(angles)
    return (
        np.concatenate([cosine, cosine], axis=1).astype(np.float32),
        np.concatenate([-sine, sine], axis=1).astype(np.float32),
    )


def dot(a, b, ca, cb):
    return lax.dot_general(a, b, (((ca,), (cb,)), ((), ())), preferred_element_type=F32)


def kernel(
    n_ctx, n_tp, blocks, hc, ht,
    lengths, queries, cotangent, keys, values, tables_in,
    att_out, gq_out, gk_out, gv_out,
    tokens, tables, firsts, stage, rfirst, ffirst, rin, kbuf, vbuf, gkbuf, gvbuf, qw, gw, ebuf, pbuf, dpbuf,
    mtile, stat, pstat, sback, fback, tback, bmain, btail,
    z_send, z_recv, relay_send, x_send, x_recv, f_send, f_recv, st_send, st_recv, bk_send, bk_recv,
    tok_sem, kv_sem, out_sem,
):
    g = min(hc, ht)
    nbc, nbt = hc // g, ht // g
    units = n_ctx * nbc
    wide = g * DH
    scale = 1.0 / math.sqrt(DH)
    me_c, me_t = lax.axis_index("ctx"), lax.axis_index("tp")
    w, n = me_t // NBR, me_t % NBR
    cos_ref, sin_ref = tables.at[0], tables.at[1]
    unroll = 4 if g % 4 == 0 else 1

    def remote(src, dst, send, recv, c, t):
        return pltpu.make_async_remote_copy(
            src_ref=src, dst_ref=dst, send_sem=send, recv_sem=recv,
            device_id={"ctx": c, "tp": t}, device_id_type=MESH,
        )

    def arrive(dst, recv):
        pltpu.make_async_copy(dst, dst, recv).wait()

    def is_me(c, t):
        return jnp.logical_and(c == me_c, t == me_t)

    def kv_copies(c):
        return (
            pltpu.make_async_copy(keys.at[c], kbuf.at[c], kv_sem.at[0, c]),
            pltpu.make_async_copy(values.at[c], vbuf.at[c], kv_sem.at[1, c]),
        )

    first_copies = (
        pltpu.make_async_copy(queries, tokens.at[0], tok_sem.at[0]),
        pltpu.make_async_copy(cotangent, tokens.at[1], tok_sem.at[1]),
        pltpu.make_async_copy(tables_in, tables, tok_sem.at[2]),
    )
    for copy in first_copies:
        copy.start()

    @pl.loop(0, n_ctx)
    def _(c):
        for copy in kv_copies(c):
            copy.start()

    barrier = pltpu.get_barrier_semaphore()

    @pl.loop(0, n_ctx * n_tp)
    def _(i):
        c, t = i // n_tp, i % n_tp

        @pl.when(jnp.logical_not(is_me(c, t)))
        def _():
            pl.semaphore_signal(barrier, inc=1, device_id={"ctx": c, "tp": t}, device_id_type=MESH)

    for copy in first_copies:
        copy.wait()

    for a in range(2):
        for j in range(blocks):
            row = tokens[a, (j + 1) * SPAN - 16 : (j + 1) * SPAN, :].astype(F32)[15:16]
            for kb in range(nbt):
                pieces = [row[:, (kb * g + i) * DH : (kb * g + i + 1) * DH] for i in range(g)]
                firsts[j, kb, a] = jnp.concatenate(pieces, axis=0).astype(BF16)

    pl.semaphore_wait(barrier, n_ctx * n_tp - 1)

    def start(src, dst, send, recv, c, t, ok):
        mine = is_me(c, t)

        @pl.when(jnp.logical_and(ok, mine))
        def _():
            pltpu.make_async_copy(src, dst, recv).start()

        @pl.when(jnp.logical_and(ok, jnp.logical_not(mine)))
        def _():
            remote(src, dst, send, recv, c, t).start()

    def sent(src, dst, send, recv, c, t, ok):
        @pl.when(jnp.logical_and(ok, jnp.logical_not(is_me(c, t))))
        def _():
            remote(src, dst, send, recv, c, t).wait_send()

    def head_block(tq, kb):
        first = tq * ht + kb * g
        return first // hc, (first % hc) // g

    def used(tw):
        return jnp.logical_not(jnp.logical_and(me_c == 0, tw == blocks - 1))

    def near(visit):
        for d in range(n_tp):
            for sign in (1, -1) if d else (1,):
                t = me_t + sign * d
                visit(jnp.clip(t, 0, n_tp - 1), jnp.logical_and(t >= 0, t < n_tp), d)

    def z_sends(act):
        def visit(t, ok, d):
            tw = t // NBR
            ok = jnp.logical_and(ok, used(tw))
            block = (tw + 1) % blocks
            rows = pl.ds(pl.multiple_of(block * SPAN, SPAN), SPAN)
            for a in range(2):
                taken = jnp.logical_or(tw == w, t % NBR == a)
                act(
                    tokens.at[a, rows], stage.at[a, me_t], z_send.at[a, t], z_recv.at[a, me_t],
                    me_c, t, jnp.logical_and(ok, taken),
                )

        near(visit)

    def f_sends(act):
        for t in range(n_tp):
            for kb in range(nbt):
                c, sb = head_block(me_t, kb)
                act(
                    firsts.at[t // NBR, kb], rfirst.at[me_c * nbc + sb], f_send.at[t, kb],
                    f_recv.at[me_c * nbc + sb], c, t, True,
                )

    slot = jnp.maximum(jnp.where(w == blocks - 1, me_c - 1, me_c), 0)
    partner = w * NBR + (NBR - 1 - n)

    def x_sends(tq, a, act, ok):
        for kb in range(nbt):
            c, sb = head_block(tq, kb)
            unit = slot * nbc + sb
            act(
                stage.at[a, tq, :, pl.ds(kb * wide, wide)], rin.at[a, unit],
                x_send.at[a, tq, kb], x_recv.at[a, unit], c, me_t, ok,
            )

    def relay(tq, a):
        return remote(stage.at[a, tq], stage.at[a, tq], relay_send.at[a, tq], z_recv.at[a, tq], me_c, partner)

    def handle(direct):
        def visit(tq, ok, d):
            ok = jnp.logical_and(ok, used(w))
            inside = tq // NBR == w
            for a in range(2):
                straight = jnp.logical_or(inside, n == a)
                now = jnp.logical_and(ok, straight if direct else jnp.logical_not(straight))

                @pl.when(now)
                def _():
                    arrive(stage.at[a, tq], z_recv.at[a, tq])

                if direct:
                    @pl.when(jnp.logical_and(now, jnp.logical_not(inside)))
                    def _():
                        relay(tq, a).start()

                x_sends(tq, a, start, now)

        near(visit)

    z_sends(start)
    f_sends(start)

    def rotated(x, rows, sign):
        turned = pltpu.roll(x, DH // 2, 1) * sin_ref[:rows]
        return x * cos_ref[:rows] + (turned if sign > 0 else -turned)

    def order(k):
        return (me_c + k) % n_ctx

    @pl.loop(0, n_ctx)
    def _(k):
        c = order(k)
        for copy in kv_copies(c):
            copy.wait()

        @pl.loop(0, hc // unroll)
        def _(hg):
            for i in range(unroll):
                h = hg * unroll + i
                x = kbuf[c, h].astype(F32)
                kbuf[c, h] = rotated(x, x.shape[0], 1).astype(BF16)

    handle(True)
    handle(False)

    lane = lax.broadcasted_iota(jnp.int32, (SPAN, DH), 1)
    row_of = lax.broadcasted_iota(jnp.int32, (SPAN, DH), 0)
    half = DH // 2

    def partner_sends(unit, act):
        for i in range(1, NBR):
            t = w * NBR + (n + i) % NBR
            copy = remote(
                stat.at[unit], pstat.at[unit, i - 1], st_send.at[unit, i - 1], st_recv.at[unit, i - 1], me_c, t
            )
            act(copy)

    @pl.loop(0, units)
    def _(k):
        c = order(k // nbc)
        sb = k % nbc
        unit = c * nbc + sb
        missing = jnp.logical_and(w == blocks - 1, c == n_ctx - 1)
        arrive(rfirst.at[unit], f_recv.at[unit])
        for a in range(2):
            ffirst[a] = rfirst[unit, a].astype(F32)

            @pl.when(jnp.logical_not(missing))
            def _():
                arrive(rin.at[a, unit], x_recv.at[a, unit])

            @pl.when(missing)
            def _():
                rin[a, unit] = jnp.zeros((SPAN, wide), BF16)

        count = lengths[c * blocks + w, n]
        live = lane[:, :] < count
        stat[unit] = jnp.zeros((SPAN, DH), F32)
        mtile[unit] = jnp.zeros((SPAN, DH), F32)

        @pl.loop(0, g // unroll)
        def _(hg):
            lps, ds, ms = [], [], []
            for i in range(unroll):
                hh = hg * unroll + i
                h = sb * g + hh
                at = c * hc + h
                columns = pl.ds(pl.multiple_of(hh * DH, DH), DH)

                def window(a):
                    raw = pltpu.roll(rin[a, unit, :, columns].astype(F32), 1, 0)
                    return jnp.where(row_of == 0, ffirst[a, pl.ds(hh, 1)], raw)

                q = rotated(window(0), SPAN, 1).astype(BF16)
                grad32 = window(1)
                grad = grad32.astype(BF16)
                qw[at] = q
                gw[at] = grad
                s = dot(q, kbuf[c, h], 1, 1) * scale
                s = jnp.where(live, s, -jnp.inf)
                m = jnp.max(s, axis=1, keepdims=True)
                e = jnp.exp(s - m)
                total = jnp.sum(e, axis=1, keepdims=True)
                value = vbuf[c, h]
                part = dot(e.astype(BF16), value, 1, 0)
                ebuf[at] = e
                pbuf[at] = part
                dpbuf[at] = dot(grad, value, 1, 1)
                lps.append(m + jnp.log(total))
                ds.append(jnp.sum(grad32 * part, axis=1, keepdims=True) / total)
                ms.append(m)
            st, mt = stat[unit], mtile[unit]
            for i in range(unroll):
                hh = hg * unroll + i
                st = jnp.where(lane == hh, lps[i], st)
                st = jnp.where(lane == hh + half, ds[i], st)
                mt = jnp.where(lane == hh, ms[i], mt)
            stat[unit] = st
            mtile[unit] = mt

        partner_sends(unit, lambda copy: copy.start())

    def back_sends(c, sb, act):
        unit = c * nbc + sb
        first = me_c * hc + sb * g
        t = first // ht
        kb = (first % ht) // g
        columns = pl.ds(pl.multiple_of(kb * wide, DH), wide)
        j = jnp.where(w == blocks - 1, 0, w + 1)
        to = jnp.where(w == blocks - 1, c + 1, c)
        for a in range(2):
            act(
                sback.at[a, unit], bmain.at[a, n, j, :, columns], bk_send.at[a, unit, 0],
                bk_recv.at[a, n, j, kb, 0], jnp.minimum(to, n_ctx - 1), t, to < n_ctx,
            )
        act(
            tback.at[unit], btail.at[n, w, kb], bk_send.at[0, unit, 1], bk_recv.at[0, n, w, kb, 1], c, t, True
        )

    def out_copies(c, sb):
        heads = pl.ds(sb * g, g)
        return (
            pltpu.make_async_copy(gkbuf.at[c, heads], gk_out.at[c, heads], out_sem.at[0, c, sb]),
            pltpu.make_async_copy(gvbuf.at[c, heads], gv_out.at[c, heads], out_sem.at[1, c, sb]),
        )

    @pl.loop(0, units)
    def _(k):
        c = order(k // nbc)
        sb = k % nbc
        unit = c * nbc + sb
        partner_sends(unit, lambda copy: copy.wait_recv())
        own = stat[unit]
        others = [pstat[unit, i] for i in range(NBR - 1)]
        top = functools.reduce(jnp.maximum, others, own)
        lse = top + jnp.log(sum(jnp.exp(x - top) for x in [own] + others))
        dots = sum(jnp.exp(x - lse) * pltpu.roll(x, half, 1) for x in [own] + others)
        factor = jnp.exp(mtile[unit] - lse)
        both = jnp.where(lane < half, factor, pltpu.roll(dots, half, 1))

        @pl.loop(0, g // unroll)
        def _(hg):
            for i in range(unroll):
                hh = hg * unroll + i
                h = sb * g + hh
                at = c * hc + h
                columns = pl.ds(pl.multiple_of(hh * DH, DH), DH)
                fac = jnp.sum(jnp.where(lane == hh, both, 0.0), axis=1, keepdims=True)
                dcol = jnp.sum(jnp.where(lane == hh + half, both, 0.0), axis=1, keepdims=True)
                pr = ebuf[at] * fac
                gvbuf[c, h] = dot(pr.astype(BF16), gw[at], 0, 0).astype(BF16)
                gs = (pr * (dpbuf[at] - dcol) * scale).astype(BF16)
                gq = dot(gs, kbuf[c, h], 1, 0)
                gk = dot(gs, qw[at], 0, 0)
                gkbuf[c, h] = rotated(gk, gk.shape[0], -1).astype(BF16)
                att = pbuf[at] * fac
                for a, x in ((0, att), (1, gq)):
                    fback[a, pl.ds(hh, 1)] = x[:1]
                    moved = jnp.where(row_of == SPAN - 1, 0.0, pltpu.roll(x, SPAN - 1, 0))
                    sback[a, unit, :, columns] = moved.astype(BF16)

        for a in range(2):
            tback[unit, a] = fback[a].astype(BF16)
        back_sends(c, sb, start)
        for copy in out_copies(c, sb):
            copy.start()

    shifted_cos = pltpu.roll(cos_ref[:SPAN], SPAN - 1, 0)
    shifted_sin = pltpu.roll(sin_ref[:SPAN], SPAN - 1, 0)
    for j in range(blocks):
        for nn in range(NBR):
            for kb in range(nbt):
                arrive(btail.at[nn, j, kb], bk_recv.at[0, nn, j, kb, 1])
                for a in range(2):
                    main = bmain.at[a, nn, j, :, pl.ds(kb * wide, wide)]
                    recv = bk_recv.at[a, nn, j, kb, 0]
                    if j > 0:
                        arrive(main, recv)
                    else:
                        @pl.when(me_c > 0)
                        def _():
                            arrive(main, recv)

                        @pl.when(me_c == 0)
                        def _():
                            bmain[a, nn, j, :, kb * wide : (kb + 1) * wide] = jnp.zeros((SPAN, wide), BF16)

        for h in range(ht):
            columns = slice(h * DH, (h + 1) * DH)

            def gathered(a):
                main = sum(bmain[a, nn, j, :, columns].astype(F32) for nn in range(NBR))
                last = sum(btail[nn, j, h // g, a].astype(F32) for nn in range(NBR))[h % g : h % g + 1]
                return jnp.where(row_of == SPAN - 1, last, main)

            rows = slice(j * SPAN, (j + 1) * SPAN)
            att_out[rows, columns] = gathered(0).astype(BF16)
            x = gathered(1)
            x = x * shifted_cos - pltpu.roll(x, DH // 2, 1) * shifted_sin
            gq_out[rows, columns] = x.astype(BF16)

    z_sends(sent)
    f_sends(sent)
    for tq in range(n_tp):
        for a in range(2):
            x_sends(tq, a, sent, used(w))

            @pl.when(jnp.logical_and(used(w), jnp.logical_and(tq // NBR != w, n == a)))
            def _():
                relay(tq, a).wait_send()

    @pl.loop(0, units)
    def _(k):
        c, sb = k // nbc, k % nbc
        partner_sends(c * nbc + sb, lambda copy: copy.wait_send())
        back_sends(c, sb, sent)
        for copy in out_copies(c, sb):
            copy.wait()


def shards(n_ctx, n_tp, queries, keys, values, cotangent, lengths):
    rows, width = queries.shape[1:]
    blocks = rows // SPAN
    ht = width // DH
    hc, neigh = keys.shape[3], keys.shape[4]
    assert keys.shape[2] == 1 and blocks * NBR == n_tp
    g = min(hc, ht)
    nbc, nbt = hc // g, ht // g
    units, wide = n_ctx * nbc, g * DH
    cosine, sine = rotation_tables(max(neigh, SPAN))
    kv_shape = (n_ctx, hc, neigh, DH)
    heads = n_ctx * hc
    any_space = pl.BlockSpec(memory_space=pl.ANY)
    vmem = pl.BlockSpec(memory_space=pltpu.VMEM)
    dma = pltpu.SemaphoreType.DMA
    att, gq, gk, gv = pl.pallas_call(
        functools.partial(kernel, n_ctx, n_tp, blocks, hc, ht),
        out_shape=(
            jax.ShapeDtypeStruct((rows, width), BF16),
            jax.ShapeDtypeStruct((rows, width), BF16),
            jax.ShapeDtypeStruct(kv_shape, BF16),
            jax.ShapeDtypeStruct(kv_shape, BF16),
        ),
        in_specs=[pl.BlockSpec(memory_space=pltpu.SMEM)] + [pl.BlockSpec(memory_space=pltpu.HBM)] * 5,
        out_specs=(vmem, vmem, any_space, any_space),
        scratch_shapes=[
            pltpu.VMEM((2, rows, width), BF16),
            pltpu.VMEM((2, max(neigh, SPAN), DH), F32),
            pltpu.VMEM((blocks, nbt, 2, g, DH), BF16),
            pltpu.VMEM((2, n_tp, SPAN, width), BF16),
            pltpu.VMEM((units, 2, g, DH), BF16),
            pltpu.VMEM((2, g, DH), F32),
            pltpu.VMEM((2, units, SPAN, wide), BF16),
            pltpu.VMEM(kv_shape, BF16),
            pltpu.VMEM(kv_shape, BF16),
            pltpu.VMEM(kv_shape, BF16),
            pltpu.VMEM(kv_shape, BF16),
            pltpu.VMEM((heads, SPAN, DH), BF16),
            pltpu.VMEM((heads, SPAN, DH), BF16),
            pltpu.VMEM((heads, SPAN, neigh), F32),
            pltpu.VMEM((heads, SPAN, DH), F32),
            pltpu.VMEM((heads, SPAN, neigh), F32),
            pltpu.VMEM((units, SPAN, DH), F32),
            pltpu.VMEM((units, SPAN, DH), F32),
            pltpu.VMEM((units, NBR - 1, SPAN, DH), F32),
            pltpu.VMEM((2, units, SPAN, wide), BF16),
            pltpu.VMEM((2, g, DH), F32),
            pltpu.VMEM((units, 2, g, DH), BF16),
            pltpu.VMEM((2, NBR, blocks, SPAN, width), BF16),
            pltpu.VMEM((NBR, blocks, nbt, 2, g, DH), BF16),
            dma((2, n_tp)),
            dma((2, n_tp)),
            dma((2, n_tp)),
            dma((2, n_tp, nbt)),
            dma((2, units)),
            dma((n_tp, nbt)),
            dma((units,)),
            dma((units, NBR - 1)),
            dma((units, NBR - 1)),
            dma((2, units, 2)),
            dma((2, NBR, blocks, nbt, 2)),
            dma((3,)),
            dma((2, n_ctx)),
            dma((2, n_ctx, nbc)),
        ],
        compiler_params=pltpu.CompilerParams(
            collective_id=0, has_side_effects=True, vmem_limit_bytes=48 * 1024 * 1024
        ),
    )(
        lengths[0].reshape(-1, NBR),
        queries[0],
        cotangent[0],
        keys.reshape(kv_shape),
        values.reshape(kv_shape),
        jnp.asarray(np.stack([cosine, sine])),
    )
    return (att[None], gq[None], gk.reshape(keys.shape), gv.reshape(values.shape))


def solution(mesh):
    tok = P("dp", "ctx", "tp")
    kv = P("dp", None, "tp", "ctx", None, None)
    return jax.shard_map(
        functools.partial(shards, mesh.shape["ctx"], mesh.shape["tp"]),
        mesh=mesh,
        in_specs=(tok, kv, kv, tok, P("dp", None, None)),
        out_specs=(tok, tok, kv, kv),
        check_vma=False,
    )
```

```python
import functools
import math

import jax
import jax.numpy as jnp
import numpy as np
from jax import lax
from jax.experimental import pallas as pl
from jax.experimental.pallas import tpu as pltpu
from jax.sharding import PartitionSpec as P

DH = 128
SPAN = 64
NBR = 2
MESH = pl.DeviceIdType.MESH
BF16 = jnp.bfloat16
F32 = jnp.float32


def rotation_tables(rows):
    frequency = 10000.0 ** (-2.0 * np.arange(DH // 2) / DH)
    frequency = frequency.astype(np.float32)
    angles = np.arange(rows, dtype=np.float32)[:, None] * frequency[None, :]
    cosine, sine = np.cos(angles), np.sin(angles)
    return (
        np.concatenate([cosine, cosine], axis=1).astype(np.float32),
        np.concatenate([-sine, sine], axis=1).astype(np.float32),
    )


def dot(a, b, ca, cb):
    return lax.dot_general(a, b, (((ca,), (cb,)), ((), ())), preferred_element_type=F32)


def kernel(
    n_ctx, n_tp, blocks, hc, ht,
    lengths, queries, cotangent, keys, values, tables_in,
    att_out, gq_out, gk_out, gv_out,
    tokens, tables, firsts, stage, rfirst, ffirst, rin, kbuf, vbuf, gkbuf, gvbuf, qw, gw, ebuf, pbuf, dpbuf,
    mtile, stat, pstat, sback, fback, tback, bstage, bmain, btail,
    z_send, z_recv, relay_send, x_send, x_recv, f_send, f_recv, st_send, st_recv, bk_send, bk_recv, bx_recv, bf_send,
    tok_sem, kv_sem, out_sem,
):
    g = min(hc, ht)
    nbc, nbt = hc // g, ht // g
    units = n_ctx * nbc
    wide = g * DH
    scale = 1.0 / math.sqrt(DH)
    me_c, me_t = lax.axis_index("ctx"), lax.axis_index("tp")
    w, n = me_t // NBR, me_t % NBR
    cos_ref, sin_ref = tables.at[0], tables.at[1]
    unroll = 4 if g % 4 == 0 else 1

    def remote(src, dst, send, recv, c, t):
        return pltpu.make_async_remote_copy(
            src_ref=src, dst_ref=dst, send_sem=send, recv_sem=recv,
            device_id={"ctx": c, "tp": t}, device_id_type=MESH,
        )

    def arrive(dst, recv):
        pltpu.make_async_copy(dst, dst, recv).wait()

    def is_me(c, t):
        return jnp.logical_and(c == me_c, t == me_t)

    def kv_copies(c):
        return (
            pltpu.make_async_copy(keys.at[c], kbuf.at[c], kv_sem.at[0, c]),
            pltpu.make_async_copy(values.at[c], vbuf.at[c], kv_sem.at[1, c]),
        )

    first_copies = (
        pltpu.make_async_copy(queries, tokens.at[0], tok_sem.at[0]),
        pltpu.make_async_copy(cotangent, tokens.at[1], tok_sem.at[1]),
        pltpu.make_async_copy(tables_in, tables, tok_sem.at[2]),
    )
    for copy in first_copies:
        copy.start()

    @pl.loop(0, n_ctx)
    def _(c):
        for copy in kv_copies(c):
            copy.start()

    barrier = pltpu.get_barrier_semaphore()

    @pl.loop(0, n_ctx * n_tp)
    def _(i):
        c, t = i // n_tp, i % n_tp

        @pl.when(jnp.logical_not(is_me(c, t)))
        def _():
            pl.semaphore_signal(barrier, inc=1, device_id={"ctx": c, "tp": t}, device_id_type=MESH)

    for copy in first_copies:
        copy.wait()

    for a in range(2):
        for j in range(blocks):
            row = tokens[a, (j + 1) * SPAN - 16 : (j + 1) * SPAN, :].astype(F32)[15:16]
            for kb in range(nbt):
                pieces = [row[:, (kb * g + i) * DH : (kb * g + i + 1) * DH] for i in range(g)]
                firsts[j, kb, a] = jnp.concatenate(pieces, axis=0).astype(BF16)

    pl.semaphore_wait(barrier, n_ctx * n_tp - 1)

    def start(src, dst, send, recv, c, t, ok):
        mine = is_me(c, t)

        @pl.when(jnp.logical_and(ok, mine))
        def _():
            pltpu.make_async_copy(src, dst, recv).start()

        @pl.when(jnp.logical_and(ok, jnp.logical_not(mine)))
        def _():
            remote(src, dst, send, recv, c, t).start()

    def sent(src, dst, send, recv, c, t, ok):
        @pl.when(jnp.logical_and(ok, jnp.logical_not(is_me(c, t))))
        def _():
            remote(src, dst, send, recv, c, t).wait_send()

    def head_block(tq, kb):
        first = tq * ht + kb * g
        return first // hc, (first % hc) // g

    def used(tw):
        return jnp.logical_not(jnp.logical_and(me_c == 0, tw == blocks - 1))

    def near(visit):
        for d in range(n_tp):
            for sign in (1, -1) if d else (1,):
                t = me_t + sign * d
                visit(jnp.clip(t, 0, n_tp - 1), jnp.logical_and(t >= 0, t < n_tp), d)

    def z_sends(act):
        def visit(t, ok, d):
            tw = t // NBR
            ok = jnp.logical_and(ok, used(tw))
            block = (tw + 1) % blocks
            rows = pl.ds(pl.multiple_of(block * SPAN, SPAN), SPAN)
            for a in range(2):
                taken = jnp.logical_or(tw == w, t % NBR == a)
                act(
                    tokens.at[a, rows], stage.at[a, me_t], z_send.at[a, t], z_recv.at[a, me_t],
                    me_c, t, jnp.logical_and(ok, taken),
                )

        near(visit)

    def f_sends(act):
        for t in range(n_tp):
            for kb in range(nbt):
                c, sb = head_block(me_t, kb)
                act(
                    firsts.at[t // NBR, kb], rfirst.at[me_c * nbc + sb], f_send.at[t, kb],
                    f_recv.at[me_c * nbc + sb], c, t, True,
                )

    slot = jnp.maximum(jnp.where(w == blocks - 1, me_c - 1, me_c), 0)
    partner = w * NBR + (NBR - 1 - n)

    def x_sends(tq, a, act, ok):
        for kb in range(nbt):
            c, sb = head_block(tq, kb)
            unit = slot * nbc + sb
            act(
                stage.at[a, tq, :, pl.ds(kb * wide, wide)], rin.at[a, unit],
                x_send.at[a, tq, kb], x_recv.at[a, unit], c, me_t, ok,
            )

    def relay(tq, a):
        return remote(stage.at[a, tq], stage.at[a, tq], relay_send.at[a, tq], z_recv.at[a, tq], me_c, partner)

    def handle(direct):
        def visit(tq, ok, d):
            ok = jnp.logical_and(ok, used(w))
            inside = tq // NBR == w
            for a in range(2):
                straight = jnp.logical_or(inside, n == a)
                now = jnp.logical_and(ok, straight if direct else jnp.logical_not(straight))

                @pl.when(now)
                def _():
                    arrive(stage.at[a, tq], z_recv.at[a, tq])

                if direct:
                    @pl.when(jnp.logical_and(now, jnp.logical_not(inside)))
                    def _():
                        relay(tq, a).start()

                x_sends(tq, a, start, now)

        near(visit)

    z_sends(start)
    f_sends(start)

    def rotated(x, rows, sign):
        turned = pltpu.roll(x, DH // 2, 1) * sin_ref[:rows]
        return x * cos_ref[:rows] + (turned if sign > 0 else -turned)

    def order(k):
        return (jnp.where(w == blocks - 1, 0, me_c) + k) % n_ctx

    @pl.loop(0, n_ctx)
    def _(k):
        c = order(k)
        for copy in kv_copies(c):
            copy.wait()

        @pl.loop(0, hc // unroll)
        def _(hg):
            for i in range(unroll):
                h = hg * unroll + i
                x = kbuf[c, h].astype(F32)
                kbuf[c, h] = rotated(x, x.shape[0], 1).astype(BF16)

    handle(True)
    handle(False)

    lane = lax.broadcasted_iota(jnp.int32, (SPAN, DH), 1)
    row_of = lax.broadcasted_iota(jnp.int32, (SPAN, DH), 0)
    half = DH // 2

    def partner_sends(unit, act):
        for i in range(1, NBR):
            t = w * NBR + (n + i) % NBR
            copy = remote(
                stat.at[unit], pstat.at[unit, i - 1], st_send.at[unit, i - 1], st_recv.at[unit, i - 1], me_c, t
            )
            act(copy)

    @pl.loop(0, units)
    def _(k):
        c = order(k // nbc)
        sb = k % nbc
        unit = c * nbc + sb
        missing = jnp.logical_and(w == blocks - 1, c == n_ctx - 1)
        arrive(rfirst.at[unit], f_recv.at[unit])
        for a in range(2):
            ffirst[a] = rfirst[unit, a].astype(F32)

            @pl.when(jnp.logical_not(missing))
            def _():
                arrive(rin.at[a, unit], x_recv.at[a, unit])

            @pl.when(missing)
            def _():
                rin[a, unit] = jnp.zeros((SPAN, wide), BF16)

        count = lengths[c * blocks + w, n]
        live = lane[:, :] < count
        stat[unit] = jnp.zeros((SPAN, DH), F32)
        mtile[unit] = jnp.zeros((SPAN, DH), F32)

        @pl.loop(0, g // unroll)
        def _(hg):
            lps, ds, ms = [], [], []
            for i in range(unroll):
                hh = hg * unroll + i
                h = sb * g + hh
                at = c * hc + h
                columns = pl.ds(pl.multiple_of(hh * DH, DH), DH)

                def window(a):
                    raw = pltpu.roll(rin[a, unit, :, columns].astype(F32), 1, 0)
                    return jnp.where(row_of == 0, ffirst[a, pl.ds(hh, 1)], raw)

                q = rotated(window(0), SPAN, 1).astype(BF16)
                grad32 = window(1)
                grad = grad32.astype(BF16)
                qw[at] = q
                gw[at] = grad
                s = dot(q, kbuf[c, h], 1, 1) * scale
                s = jnp.where(live, s, -jnp.inf)
                m = jnp.max(s, axis=1, keepdims=True)
                e = jnp.exp(s - m)
                total = jnp.sum(e, axis=1, keepdims=True)
                value = vbuf[c, h]
                part = dot(e.astype(BF16), value, 1, 0)
                ebuf[at] = e
                pbuf[at] = part
                dpbuf[at] = dot(grad, value, 1, 1)
                lps.append(m + jnp.log(total))
                ds.append(jnp.sum(grad32 * part, axis=1, keepdims=True) / total)
                ms.append(m)
            st, mt = stat[unit], mtile[unit]
            for i in range(unroll):
                hh = hg * unroll + i
                st = jnp.where(lane == hh, lps[i], st)
                st = jnp.where(lane == hh + half, ds[i], st)
                mt = jnp.where(lane == hh, ms[i], mt)
            stat[unit] = st
            mtile[unit] = mt

        partner_sends(unit, lambda copy: copy.start())

    def back_sends(c, sb, act):
        unit = c * nbc + sb
        first = me_c * hc + sb * g
        t = first // ht
        kb = (first % ht) // g
        columns = pl.ds(pl.multiple_of(kb * wide, DH), wide)
        j = jnp.where(w == blocks - 1, 0, w + 1)
        to = jnp.where(w == blocks - 1, c + 1, c)
        for a in range(2):
            act(
                sback.at[a, unit], bmain.at[a, n, j, :, columns], bk_send.at[a, unit, 0],
                bk_recv.at[a, n, j, kb, 0], me_c, t, to == me_c,
            )
            act(
                sback.at[a, unit], bstage.at[a, t, :, columns], bk_send.at[a, unit, 0],
                bx_recv.at[a, t, kb], jnp.minimum(to, n_ctx - 1), me_t,
                jnp.logical_and(to < n_ctx, to != me_c),
            )
        act(
            tback.at[unit], btail.at[n, w, kb], bk_send.at[0, unit, 1], bk_recv.at[0, n, w, kb, 1], c, t, True
        )

    def back_forward(tq, act):
        j = jnp.where(w == blocks - 1, 0, w + 1)
        for kb in range(nbt):
            columns = pl.ds(kb * wide, wide)
            ok = jnp.logical_and(used(w), head_block(tq, kb)[0] != me_c)
            for a in range(2):
                act(
                    bstage.at[a, tq, :, columns], bmain.at[a, n, j, :, columns], bf_send.at[a, tq, kb],
                    bk_recv.at[a, n, j, kb, 0], me_c, tq, ok,
                )

    def out_copies(c, sb):
        heads = pl.ds(sb * g, g)
        return (
            pltpu.make_async_copy(gkbuf.at[c, heads], gk_out.at[c, heads], out_sem.at[0, c, sb]),
            pltpu.make_async_copy(gvbuf.at[c, heads], gv_out.at[c, heads], out_sem.at[1, c, sb]),
        )

    @pl.loop(0, units)
    def _(k):
        c = order(k // nbc)
        sb = k % nbc
        unit = c * nbc + sb
        partner_sends(unit, lambda copy: copy.wait_recv())
        own = stat[unit]
        others = [pstat[unit, i] for i in range(NBR - 1)]
        top = functools.reduce(jnp.maximum, others, own)
        lse = top + jnp.log(sum(jnp.exp(x - top) for x in [own] + others))
        dots = sum(jnp.exp(x - lse) * pltpu.roll(x, half, 1) for x in [own] + others)
        factor = jnp.exp(mtile[unit] - lse)
        both = jnp.where(lane < half, factor, pltpu.roll(dots, half, 1))

        @pl.loop(0, g // unroll)
        def _(hg):
            for i in range(unroll):
                hh = hg * unroll + i
                h = sb * g + hh
                at = c * hc + h
                columns = pl.ds(pl.multiple_of(hh * DH, DH), DH)
                fac = jnp.sum(jnp.where(lane == hh, both, 0.0), axis=1, keepdims=True)
                dcol = jnp.sum(jnp.where(lane == hh + half, both, 0.0), axis=1, keepdims=True)
                pr = ebuf[at] * fac
                gvbuf[c, h] = dot(pr.astype(BF16), gw[at], 0, 0).astype(BF16)
                gs = (pr * (dpbuf[at] - dcol) * scale).astype(BF16)
                gq = dot(gs, kbuf[c, h], 1, 0)
                gk = dot(gs, qw[at], 0, 0)
                gkbuf[c, h] = rotated(gk, gk.shape[0], -1).astype(BF16)
                att = pbuf[at] * fac
                for a, x in ((0, att), (1, gq)):
                    fback[a, pl.ds(hh, 1)] = x[:1]
                    moved = jnp.where(row_of == SPAN - 1, 0.0, pltpu.roll(x, SPAN - 1, 0))
                    sback[a, unit, :, columns] = moved.astype(BF16)

        for a in range(2):
            tback[unit, a] = fback[a].astype(BF16)
        back_sends(c, sb, start)
        for copy in out_copies(c, sb):
            copy.start()

    for tq in range(n_tp):
        for kb in range(nbt):
            ok = jnp.logical_and(used(w), head_block(tq, kb)[0] != me_c)

            @pl.when(ok)
            def _():
                for a in range(2):
                    arrive(bstage.at[a, tq, :, pl.ds(kb * wide, wide)], bx_recv.at[a, tq, kb])

        back_forward(tq, start)

    shifted_cos = pltpu.roll(cos_ref[:SPAN], SPAN - 1, 0)
    shifted_sin = pltpu.roll(sin_ref[:SPAN], SPAN - 1, 0)
    for j in range(blocks):
        for nn in range(NBR):
            for kb in range(nbt):
                arrive(btail.at[nn, j, kb], bk_recv.at[0, nn, j, kb, 1])
                for a in range(2):
                    main = bmain.at[a, nn, j, :, pl.ds(kb * wide, wide)]
                    recv = bk_recv.at[a, nn, j, kb, 0]
                    if j > 0:
                        arrive(main, recv)
                    else:
                        @pl.when(me_c > 0)
                        def _():
                            arrive(main, recv)

                        @pl.when(me_c == 0)
                        def _():
                            bmain[a, nn, j, :, kb * wide : (kb + 1) * wide] = jnp.zeros((SPAN, wide), BF16)

        for h in range(ht):
            columns = slice(h * DH, (h + 1) * DH)

            def gathered(a):
                main = sum(bmain[a, nn, j, :, columns].astype(F32) for nn in range(NBR))
                last = sum(btail[nn, j, h // g, a].astype(F32) for nn in range(NBR))[h % g : h % g + 1]
                return jnp.where(row_of == SPAN - 1, last, main)

            rows = slice(j * SPAN, (j + 1) * SPAN)
            att_out[rows, columns] = gathered(0).astype(BF16)
            x = gathered(1)
            x = x * shifted_cos - pltpu.roll(x, DH // 2, 1) * shifted_sin
            gq_out[rows, columns] = x.astype(BF16)

    z_sends(sent)
    f_sends(sent)
    for tq in range(n_tp):
        back_forward(tq, sent)
    for tq in range(n_tp):
        for a in range(2):
            x_sends(tq, a, sent, used(w))

            @pl.when(jnp.logical_and(used(w), jnp.logical_and(tq // NBR != w, n == a)))
            def _():
                relay(tq, a).wait_send()

    @pl.loop(0, units)
    def _(k):
        c, sb = k // nbc, k % nbc
        partner_sends(c * nbc + sb, lambda copy: copy.wait_send())
        back_sends(c, sb, sent)
        for copy in out_copies(c, sb):
            copy.wait()


def shards(n_ctx, n_tp, queries, keys, values, cotangent, lengths):
    rows, width = queries.shape[1:]
    blocks = rows // SPAN
    ht = width // DH
    hc, neigh = keys.shape[3], keys.shape[4]
    assert keys.shape[2] == 1 and blocks * NBR == n_tp
    g = min(hc, ht)
    nbc, nbt = hc // g, ht // g
    units, wide = n_ctx * nbc, g * DH
    cosine, sine = rotation_tables(max(neigh, SPAN))
    kv_shape = (n_ctx, hc, neigh, DH)
    heads = n_ctx * hc
    any_space = pl.BlockSpec(memory_space=pl.ANY)
    vmem = pl.BlockSpec(memory_space=pltpu.VMEM)
    dma = pltpu.SemaphoreType.DMA
    att, gq, gk, gv = pl.pallas_call(
        functools.partial(kernel, n_ctx, n_tp, blocks, hc, ht),
        out_shape=(
            jax.ShapeDtypeStruct((rows, width), BF16),
            jax.ShapeDtypeStruct((rows, width), BF16),
            jax.ShapeDtypeStruct(kv_shape, BF16),
            jax.ShapeDtypeStruct(kv_shape, BF16),
        ),
        in_specs=[pl.BlockSpec(memory_space=pltpu.SMEM)] + [pl.BlockSpec(memory_space=pltpu.HBM)] * 5,
        out_specs=(vmem, vmem, any_space, any_space),
        scratch_shapes=[
            pltpu.VMEM((2, rows, width), BF16),
            pltpu.VMEM((2, max(neigh, SPAN), DH), F32),
            pltpu.VMEM((blocks, nbt, 2, g, DH), BF16),
            pltpu.VMEM((2, n_tp, SPAN, width), BF16),
            pltpu.VMEM((units, 2, g, DH), BF16),
            pltpu.VMEM((2, g, DH), F32),
            pltpu.VMEM((2, units, SPAN, wide), BF16),
            pltpu.VMEM(kv_shape, BF16),
            pltpu.VMEM(kv_shape, BF16),
            pltpu.VMEM(kv_shape, BF16),
            pltpu.VMEM(kv_shape, BF16),
            pltpu.VMEM((heads, SPAN, DH), BF16),
            pltpu.VMEM((heads, SPAN, DH), BF16),
            pltpu.VMEM((heads, SPAN, neigh), F32),
            pltpu.VMEM((heads, SPAN, DH), F32),
            pltpu.VMEM((heads, SPAN, neigh), F32),
            pltpu.VMEM((units, SPAN, DH), F32),
            pltpu.VMEM((units, SPAN, DH), F32),
            pltpu.VMEM((units, NBR - 1, SPAN, DH), F32),
            pltpu.VMEM((2, units, SPAN, wide), BF16),
            pltpu.VMEM((2, g, DH), F32),
            pltpu.VMEM((units, 2, g, DH), BF16),
            pltpu.VMEM((2, n_tp, SPAN, width), BF16),
            pltpu.VMEM((2, NBR, blocks, SPAN, width), BF16),
            pltpu.VMEM((NBR, blocks, nbt, 2, g, DH), BF16),
            dma((2, n_tp)),
            dma((2, n_tp)),
            dma((2, n_tp)),
            dma((2, n_tp, nbt)),
            dma((2, units)),
            dma((n_tp, nbt)),
            dma((units,)),
            dma((units, NBR - 1)),
            dma((units, NBR - 1)),
            dma((2, units, 2)),
            dma((2, NBR, blocks, nbt, 2)),
            dma((2, n_tp, nbt)),
            dma((2, n_tp, nbt)),
            dma((3,)),
            dma((2, n_ctx)),
            dma((2, n_ctx, nbc)),
        ],
        compiler_params=pltpu.CompilerParams(
            collective_id=0, has_side_effects=True, vmem_limit_bytes=48 * 1024 * 1024
        ),
    )(
        lengths[0].reshape(-1, NBR),
        queries[0],
        cotangent[0],
        keys.reshape(kv_shape),
        values.reshape(kv_shape),
        jnp.asarray(np.stack([cosine, sine])),
    )
    return (att[None], gq[None], gk.reshape(keys.shape), gv.reshape(values.shape))


def solution(mesh):
    tok = P("dp", "ctx", "tp")
    kv = P("dp", None, "tp", "ctx", None, None)
    return jax.shard_map(
        functools.partial(shards, mesh.shape["ctx"], mesh.shape["tp"]),
        mesh=mesh,
        in_specs=(tok, kv, kv, tok, P("dp", None, None)),
        out_specs=(tok, tok, kv, kv),
        check_vma=False,
    )
```

```python
import functools
import math

import jax
import jax.numpy as jnp
import numpy as np
from jax import lax
from jax.experimental import pallas as pl
from jax.experimental.pallas import tpu as pltpu
from jax.sharding import PartitionSpec as P

DH = 128
SPAN = 64
NBR = 2
MESH = pl.DeviceIdType.MESH
BF16 = jnp.bfloat16
F32 = jnp.float32


def rotation_tables(rows):
    frequency = 10000.0 ** (-2.0 * np.arange(DH // 2) / DH)
    frequency = frequency.astype(np.float32)
    angles = np.arange(rows, dtype=np.float32)[:, None] * frequency[None, :]
    cosine, sine = np.cos(angles), np.sin(angles)
    return (
        np.concatenate([cosine, cosine], axis=1).astype(np.float32),
        np.concatenate([-sine, sine], axis=1).astype(np.float32),
    )


def dot(a, b, ca, cb):
    return lax.dot_general(a, b, (((ca,), (cb,)), ((), ())), preferred_element_type=F32)


def kernel(
    n_ctx, n_tp, blocks, hc, ht,
    lengths, queries, cotangent, keys, values, tables_in,
    att_out, gq_out, gk_out, gv_out,
    tokens, tables, firsts, stage, rfirst, ffirst, rin, kbuf, vbuf, gkbuf, gvbuf, qw, gw, ebuf, pbuf, dpbuf,
    mtile, stat, pstat, sback, fback, tback, bstage, bmain, btail,
    z_send, z_recv, relay_send, x_send, x_recv, f_send, f_recv, st_send, st_recv, bk_send, bk_recv, bx_recv, bf_send,
    tok_sem, kv_sem, out_sem,
):
    g = min(hc, ht)
    nbc, nbt = hc // g, ht // g
    units = n_ctx * nbc
    wide = g * DH
    scale = 1.0 / math.sqrt(DH)
    me_c, me_t = lax.axis_index("ctx"), lax.axis_index("tp")
    w, n = me_t // NBR, me_t % NBR
    cos_ref, sin_ref = tables.at[0], tables.at[1]
    unroll = 4 if g % 4 == 0 else 1

    def remote(src, dst, send, recv, c, t):
        return pltpu.make_async_remote_copy(
            src_ref=src, dst_ref=dst, send_sem=send, recv_sem=recv,
            device_id={"ctx": c, "tp": t}, device_id_type=MESH,
        )

    def arrive(dst, recv):
        pltpu.make_async_copy(dst, dst, recv).wait()

    def is_me(c, t):
        return jnp.logical_and(c == me_c, t == me_t)

    def kv_copies(c):
        return (
            pltpu.make_async_copy(keys.at[c], kbuf.at[c], kv_sem.at[0, c]),
            pltpu.make_async_copy(values.at[c], vbuf.at[c], kv_sem.at[1, c]),
        )

    first_copies = (
        pltpu.make_async_copy(queries, tokens.at[0], tok_sem.at[0]),
        pltpu.make_async_copy(cotangent, tokens.at[1], tok_sem.at[1]),
        pltpu.make_async_copy(tables_in, tables, tok_sem.at[2]),
    )
    for copy in first_copies:
        copy.start()

    @pl.loop(0, n_ctx)
    def _(c):
        for copy in kv_copies(c):
            copy.start()

    barrier = pltpu.get_barrier_semaphore()

    @pl.loop(0, n_ctx * n_tp)
    def _(i):
        c, t = i // n_tp, i % n_tp

        @pl.when(jnp.logical_not(is_me(c, t)))
        def _():
            pl.semaphore_signal(barrier, inc=1, device_id={"ctx": c, "tp": t}, device_id_type=MESH)

    for copy in first_copies:
        copy.wait()

    for a in range(2):
        for j in range(blocks):
            row = tokens[a, (j + 1) * SPAN - 16 : (j + 1) * SPAN, :].astype(F32)[15:16]
            for kb in range(nbt):
                pieces = [row[:, (kb * g + i) * DH : (kb * g + i + 1) * DH] for i in range(g)]
                firsts[j, kb, a] = jnp.concatenate(pieces, axis=0).astype(BF16)

    pl.semaphore_wait(barrier, n_ctx * n_tp - 1)

    def start(src, dst, send, recv, c, t, ok):
        mine = is_me(c, t)

        @pl.when(jnp.logical_and(ok, mine))
        def _():
            pltpu.make_async_copy(src, dst, recv).start()

        @pl.when(jnp.logical_and(ok, jnp.logical_not(mine)))
        def _():
            remote(src, dst, send, recv, c, t).start()

    def sent(src, dst, send, recv, c, t, ok):
        @pl.when(jnp.logical_and(ok, jnp.logical_not(is_me(c, t))))
        def _():
            remote(src, dst, send, recv, c, t).wait_send()

    def head_block(tq, kb):
        first = tq * ht + kb * g
        return first // hc, (first % hc) // g

    def used(tw):
        return jnp.logical_not(jnp.logical_and(me_c == 0, tw == blocks - 1))

    def near(visit):
        for d in range(n_tp):
            for sign in (1, -1) if d else (1,):
                t = me_t + sign * d
                visit(jnp.clip(t, 0, n_tp - 1), jnp.logical_and(t >= 0, t < n_tp), d)

    def z_sends(act):
        def visit(t, ok, d):
            tw = t // NBR
            ok = jnp.logical_and(ok, used(tw))
            block = (tw + 1) % blocks
            rows = pl.ds(pl.multiple_of(block * SPAN, SPAN), SPAN)
            for a in range(2):
                taken = jnp.logical_or(tw == w, t % NBR == a)
                act(
                    tokens.at[a, rows], stage.at[a, me_t], z_send.at[a, t], z_recv.at[a, me_t],
                    me_c, t, jnp.logical_and(ok, taken),
                )

        near(visit)

    def f_sends(act):
        for t in range(n_tp):
            for kb in range(nbt):
                c, sb = head_block(me_t, kb)
                act(
                    firsts.at[t // NBR, kb], rfirst.at[me_c * nbc + sb], f_send.at[t, kb],
                    f_recv.at[me_c * nbc + sb], c, t, True,
                )

    slot = jnp.maximum(jnp.where(w == blocks - 1, me_c - 1, me_c), 0)
    partner = w * NBR + (NBR - 1 - n)

    def x_sends(tq, a, act, ok):
        for kb in range(nbt):
            c, sb = head_block(tq, kb)
            unit = slot * nbc + sb
            act(
                stage.at[a, tq, :, pl.ds(kb * wide, wide)], rin.at[a, unit],
                x_send.at[a, tq, kb], x_recv.at[a, unit], c, me_t, ok,
            )

    def relay(tq, a):
        return remote(stage.at[a, tq], stage.at[a, tq], relay_send.at[a, tq], z_recv.at[a, tq], me_c, partner)

    def handle(direct):
        def visit(tq, ok, d):
            ok = jnp.logical_and(ok, used(w))
            inside = tq // NBR == w
            for a in range(2):
                straight = jnp.logical_or(inside, n == a)
                now = jnp.logical_and(ok, straight if direct else jnp.logical_not(straight))

                @pl.when(now)
                def _():
                    arrive(stage.at[a, tq], z_recv.at[a, tq])

                if direct:
                    @pl.when(jnp.logical_and(now, jnp.logical_not(inside)))
                    def _():
                        relay(tq, a).start()

                x_sends(tq, a, start, now)

        near(visit)

    z_sends(start)
    f_sends(start)

    def rotated(x, rows, sign):
        turned = pltpu.roll(x, DH // 2, 1) * sin_ref[:rows]
        return x * cos_ref[:rows] + (turned if sign > 0 else -turned)

    def order(k):
        return (jnp.where(w == blocks - 1, 0, me_c) + k) % n_ctx

    @pl.loop(0, n_ctx)
    def _(k):
        c = order(k)
        for copy in kv_copies(c):
            copy.wait()

        @pl.loop(0, hc // unroll)
        def _(hg):
            for i in range(unroll):
                h = hg * unroll + i
                x = kbuf[c, h].astype(F32)
                kbuf[c, h] = rotated(x, x.shape[0], 1).astype(BF16)

    handle(True)
    handle(False)

    lane = lax.broadcasted_iota(jnp.int32, (SPAN, DH), 1)
    row_of = lax.broadcasted_iota(jnp.int32, (SPAN, DH), 0)
    half = DH // 2

    def partner_sends(unit, act):
        for i in range(1, NBR):
            t = w * NBR + (n + i) % NBR
            copy = remote(
                stat.at[unit], pstat.at[unit, i - 1], st_send.at[unit, i - 1], st_recv.at[unit, i - 1], me_c, t
            )
            act(copy)

    @pl.loop(0, units)
    def _(k):
        c = order(k // nbc)
        sb = k % nbc
        unit = c * nbc + sb
        missing = jnp.logical_and(w == blocks - 1, c == n_ctx - 1)
        arrive(rfirst.at[unit], f_recv.at[unit])
        for a in range(2):
            ffirst[a] = rfirst[unit, a].astype(F32)

            @pl.when(jnp.logical_not(missing))
            def _():
                arrive(rin.at[a, unit], x_recv.at[a, unit])

            @pl.when(missing)
            def _():
                rin[a, unit] = jnp.zeros((SPAN, wide), BF16)

        count = lengths[c * blocks + w, n]
        live = lane[:, :] < count
        stat[unit] = jnp.zeros((SPAN, DH), F32)
        mtile[unit] = jnp.zeros((SPAN, DH), F32)

        @pl.loop(0, g // unroll)
        def _(hg):
            lps, ds, ms = [], [], []
            for i in range(unroll):
                hh = hg * unroll + i
                h = sb * g + hh
                at = c * hc + h
                columns = pl.ds(pl.multiple_of(hh * DH, DH), DH)

                def window(a):
                    raw = pltpu.roll(rin[a, unit, :, columns].astype(F32), 1, 0)
                    return jnp.where(row_of == 0, ffirst[a, pl.ds(hh, 1)], raw)

                q = rotated(window(0), SPAN, 1).astype(BF16)
                grad32 = window(1)
                grad = grad32.astype(BF16)
                qw[at] = q
                gw[at] = grad
                s = dot(q, kbuf[c, h], 1, 1) * scale
                s = jnp.where(live, s, -jnp.inf)
                m = jnp.max(s, axis=1, keepdims=True)
                e = jnp.exp(s - m)
                total = jnp.sum(e, axis=1, keepdims=True)
                value = vbuf[c, h]
                part = dot(e.astype(BF16), value, 1, 0)
                ebuf[at] = e
                pbuf[at] = part
                dpbuf[at] = dot(grad, value, 1, 1)
                lps.append(m + jnp.log(total))
                ds.append(jnp.sum(grad32 * part, axis=1, keepdims=True) / total)
                ms.append(m)
            st, mt = stat[unit], mtile[unit]
            for i in range(unroll):
                hh = hg * unroll + i
                st = jnp.where(lane == hh, lps[i], st)
                st = jnp.where(lane == hh + half, ds[i], st)
                mt = jnp.where(lane == hh, ms[i], mt)
            stat[unit] = st
            mtile[unit] = mt

        partner_sends(unit, lambda copy: copy.start())

    def back_sends(c, sb, act):
        unit = c * nbc + sb
        first = me_c * hc + sb * g
        t = first // ht
        kb = (first % ht) // g
        columns = pl.ds(pl.multiple_of(kb * wide, DH), wide)
        j = jnp.where(w == blocks - 1, 0, w + 1)
        to = jnp.where(w == blocks - 1, c + 1, c)
        for a in range(2):
            act(
                sback.at[a, unit], bmain.at[a, n, j, :, columns], bk_send.at[a, unit, 0],
                bk_recv.at[a, n, j, kb, 0], me_c, t, to == me_c,
            )
            act(
                sback.at[a, unit], bstage.at[a, t, :, columns], bk_send.at[a, unit, 0],
                bx_recv.at[a, t, kb], jnp.minimum(to, n_ctx - 1), me_t,
                jnp.logical_and(to < n_ctx, to != me_c),
            )
        act(
            tback.at[unit], btail.at[n, w, kb], bk_send.at[0, unit, 1], bk_recv.at[0, n, w, kb, 1], c, t, True
        )

    def back_forward(tq, act):
        j = jnp.where(w == blocks - 1, 0, w + 1)
        for kb in range(nbt):
            columns = pl.ds(kb * wide, wide)
            ok = jnp.logical_and(used(w), head_block(tq, kb)[0] != me_c)
            for a in range(2):
                act(
                    bstage.at[a, tq, :, columns], bmain.at[a, n, j, :, columns], bf_send.at[a, tq, kb],
                    bk_recv.at[a, n, j, kb, 0], me_c, tq, ok,
                )

    def out_copies(c, sb):
        heads = pl.ds(sb * g, g)
        return (
            pltpu.make_async_copy(gkbuf.at[c, heads], gk_out.at[c, heads], out_sem.at[0, c, sb]),
            pltpu.make_async_copy(gvbuf.at[c, heads], gv_out.at[c, heads], out_sem.at[1, c, sb]),
        )

    @pl.loop(0, units)
    def _(k):
        c = order(k // nbc)
        sb = k % nbc
        unit = c * nbc + sb
        partner_sends(unit, lambda copy: copy.wait_recv())
        own = stat[unit]
        others = [pstat[unit, i] for i in range(NBR - 1)]
        top = functools.reduce(jnp.maximum, others, own)
        lse = top + jnp.log(sum(jnp.exp(x - top) for x in [own] + others))
        dots = sum(jnp.exp(x - lse) * pltpu.roll(x, half, 1) for x in [own] + others)
        factor = jnp.exp(mtile[unit] - lse)
        both = jnp.where(lane < half, factor, pltpu.roll(dots, half, 1))

        @pl.loop(0, g // unroll)
        def _(hg):
            for i in range(unroll):
                hh = hg * unroll + i
                h = sb * g + hh
                at = c * hc + h
                columns = pl.ds(pl.multiple_of(hh * DH, DH), DH)
                fac = jnp.sum(jnp.where(lane == hh, both, 0.0), axis=1, keepdims=True)
                dcol = jnp.sum(jnp.where(lane == hh + half, both, 0.0), axis=1, keepdims=True)
                pr = ebuf[at] * fac
                gvbuf[c, h] = dot(pr.astype(BF16), gw[at], 0, 0).astype(BF16)
                gs = (pr * (dpbuf[at] - dcol) * scale).astype(BF16)
                gq = dot(gs, kbuf[c, h], 1, 0)
                gk = dot(gs, qw[at], 0, 0)
                gkbuf[c, h] = rotated(gk, gk.shape[0], -1).astype(BF16)
                att = pbuf[at] * fac
                for a, x in ((0, att), (1, gq)):
                    fback[a, pl.ds(hh, 1)] = x[:1]
                    moved = jnp.where(row_of == SPAN - 1, 0.0, pltpu.roll(x, SPAN - 1, 0))
                    sback[a, unit, :, columns] = moved.astype(BF16)

        for a in range(2):
            tback[unit, a] = fback[a].astype(BF16)
        back_sends(c, sb, start)
        for copy in out_copies(c, sb):
            copy.start()

    for tq in range(n_tp):
        for kb in range(nbt):
            ok = jnp.logical_and(used(w), head_block(tq, kb)[0] != me_c)

            @pl.when(ok)
            def _():
                for a in range(2):
                    arrive(bstage.at[a, tq, :, pl.ds(kb * wide, wide)], bx_recv.at[a, tq, kb])

        back_forward(tq, start)

    shifted_cos = pltpu.roll(cos_ref[:SPAN], SPAN - 1, 0)
    shifted_sin = pltpu.roll(sin_ref[:SPAN], SPAN - 1, 0)
    for j in range(blocks):
        for nn in range(NBR):
            for kb in range(nbt):
                arrive(btail.at[nn, j, kb], bk_recv.at[0, nn, j, kb, 1])
                for a in range(2):
                    main = bmain.at[a, nn, j, :, pl.ds(kb * wide, wide)]
                    recv = bk_recv.at[a, nn, j, kb, 0]
                    if j > 0:
                        arrive(main, recv)
                    else:
                        @pl.when(me_c > 0)
                        def _():
                            arrive(main, recv)

                        @pl.when(me_c == 0)
                        def _():
                            bmain[a, nn, j, :, kb * wide : (kb + 1) * wide] = jnp.zeros((SPAN, wide), BF16)

        for h in range(ht):
            columns = slice(h * DH, (h + 1) * DH)

            def gathered(a):
                main = sum(bmain[a, nn, j, :, columns].astype(F32) for nn in range(NBR))
                last = sum(btail[nn, j, h // g, a].astype(F32) for nn in range(NBR))[h % g : h % g + 1]
                return jnp.where(row_of == SPAN - 1, last, main)

            rows = slice(j * SPAN, (j + 1) * SPAN)
            att_out[rows, columns] = gathered(0).astype(BF16)
            x = gathered(1)
            x = x * shifted_cos - pltpu.roll(x, DH // 2, 1) * shifted_sin
            gq_out[rows, columns] = x.astype(BF16)

    z_sends(sent)
    f_sends(sent)
    for tq in range(n_tp):
        back_forward(tq, sent)
    for tq in range(n_tp):
        for a in range(2):
            x_sends(tq, a, sent, used(w))

            @pl.when(jnp.logical_and(used(w), jnp.logical_and(tq // NBR != w, n == a)))
            def _():
                relay(tq, a).wait_send()

    @pl.loop(0, units)
    def _(k):
        c, sb = k // nbc, k % nbc
        partner_sends(c * nbc + sb, lambda copy: copy.wait_send())
        back_sends(c, sb, sent)
        for copy in out_copies(c, sb):
            copy.wait()


def shards(n_ctx, n_tp, queries, keys, values, cotangent, lengths):
    rows, width = queries.shape[1:]
    blocks = rows // SPAN
    ht = width // DH
    hc, neigh = keys.shape[3], keys.shape[4]
    assert keys.shape[2] == 1 and blocks * NBR == n_tp
    g = min(hc, ht)
    nbc, nbt = hc // g, ht // g
    units, wide = n_ctx * nbc, g * DH
    cosine, sine = rotation_tables(max(neigh, SPAN))
    kv_shape = (n_ctx, hc, neigh, DH)
    heads = n_ctx * hc
    any_space = pl.BlockSpec(memory_space=pl.ANY)
    vmem = pl.BlockSpec(memory_space=pltpu.VMEM)
    dma = pltpu.SemaphoreType.DMA
    att, gq, gk, gv = pl.pallas_call(
        functools.partial(kernel, n_ctx, n_tp, blocks, hc, ht),
        out_shape=(
            jax.ShapeDtypeStruct((rows, width), BF16),
            jax.ShapeDtypeStruct((rows, width), BF16),
            jax.ShapeDtypeStruct(kv_shape, BF16),
            jax.ShapeDtypeStruct(kv_shape, BF16),
        ),
        in_specs=[pl.BlockSpec(memory_space=pltpu.SMEM)] + [pl.BlockSpec(memory_space=pltpu.HBM)] * 5,
        out_specs=(vmem, vmem, any_space, any_space),
        scratch_shapes=[
            pltpu.VMEM((2, rows, width), BF16),
            pltpu.VMEM((2, max(neigh, SPAN), DH), F32),
            pltpu.VMEM((blocks, nbt, 2, g, DH), BF16),
            pltpu.VMEM((2, n_tp, SPAN, width), BF16),
            pltpu.VMEM((units, 2, g, DH), BF16),
            pltpu.VMEM((2, g, DH), F32),
            pltpu.VMEM((2, units, SPAN, wide), BF16),
            pltpu.VMEM(kv_shape, BF16),
            pltpu.VMEM(kv_shape, BF16),
            pltpu.VMEM(kv_shape, BF16),
            pltpu.VMEM(kv_shape, BF16),
            pltpu.VMEM((heads, SPAN, DH), BF16),
            pltpu.VMEM((heads, SPAN, DH), BF16),
            pltpu.VMEM((heads, SPAN, neigh), F32),
            pltpu.VMEM((heads, SPAN, DH), F32),
            pltpu.VMEM((heads, SPAN, neigh), F32),
            pltpu.VMEM((units, SPAN, DH), F32),
            pltpu.VMEM((units, SPAN, DH), F32),
            pltpu.VMEM((units, NBR - 1, SPAN, DH), F32),
            pltpu.VMEM((2, units, SPAN, wide), BF16),
            pltpu.VMEM((2, g, DH), F32),
            pltpu.VMEM((units, 2, g, DH), BF16),
            pltpu.VMEM((2, n_tp, SPAN, width), BF16),
            pltpu.VMEM((2, NBR, blocks, SPAN, width), BF16),
            pltpu.VMEM((NBR, blocks, nbt, 2, g, DH), BF16),
            dma((2, n_tp)),
            dma((2, n_tp)),
            dma((2, n_tp)),
            dma((2, n_tp, nbt)),
            dma((2, units)),
            dma((n_tp, nbt)),
            dma((units,)),
            dma((units, NBR - 1)),
            dma((units, NBR - 1)),
            dma((2, units, 2)),
            dma((2, NBR, blocks, nbt, 2)),
            dma((2, n_tp, nbt)),
            dma((2, n_tp, nbt)),
            dma((3,)),
            dma((2, n_ctx)),
            dma((2, n_ctx, nbc)),
        ],
        compiler_params=pltpu.CompilerParams(
            collective_id=0, has_side_effects=True, vmem_limit_bytes=61 * 1024 * 1024
        ),
    )(
        lengths[0].reshape(-1, NBR),
        queries[0],
        cotangent[0],
        keys.reshape(kv_shape),
        values.reshape(kv_shape),
        jnp.asarray(np.stack([cosine, sine])),
    )
    return (att[None], gq[None], gk.reshape(keys.shape), gv.reshape(values.shape))


def solution(mesh):
    tok = P("dp", "ctx", "tp")
    kv = P("dp", None, "tp", "ctx", None, None)
    return jax.shard_map(
        functools.partial(shards, mesh.shape["ctx"], mesh.shape["tp"]),
        mesh=mesh,
        in_specs=(tok, kv, kv, tok, P("dp", None, None)),
        out_specs=(tok, tok, kv, kv),
        check_vma=False,
    )
```
